32 devices in a mesh: dp: 8 (over z, x), txt: 4 (over y, core).
Axes of the slice: x: 2, y: 2, z: 4, core: 2. Of those that a mesh axis runs over, the one named last changes fastest.
Arguments:
- resid: bfloat16 [2048, 1024], P('dp', 'txt'), may hold values from -40 to 40
- prenorm_gain: float32 [1024], replicated, may hold values from 0.25 to 1.75
- prenorm_bias: float32 [1024], replicated, may hold values from -3 to 3
- up_weight: bfloat16 [1024, 4096], P('dp', 'txt'), may hold values from -0.1875 to 0.1875
- up_bias: float32 [4096], P('txt'), may hold values from -3 to 3
- down_weight: bfloat16 [4096, 1024], P('txt', 'dp'), may hold values from -0.09375 to 0.09375
- down_bias: float32 [1024], replicated, may hold values from -3 to 3
- post_gain: float32 [1024], P('txt'), may hold values from 0.25 to 1.75
- post_bias: float32 [1024], P('txt'), may hold values from -3 to 3
- projection: bfloat16 [1024, 768], P('txt'), may hold values from -1 to 1
- texts: bfloat16 [5120, 768], P('txt'), may hold values from -48 to 48
- labels: int32 [2048], P('dp'), may hold values from 0 to 5119
- step_size: float32 [1], replicated, may hold values from 0.5 to 2
Outputs:
- adversarial: float32 [2048, 1024], P('dp', 'txt')
The draws below stay inside these ranges and needn't reach their ends.
All inputs are finite; a program needn't handle non-finite values.
Results may differ from the reference program's by a relative error of at most 0.0036.
Values may be sent and summed in bfloat16 or wider, within the bound.
A program may use at most 64 MiB of HBM per device.

```python
import math
import jax
import jax.numpy as jnp
from jax import lax

MODEL_WIDTH = 1024
FF = 4096
E = 768
IMG_DEV = 256
IMAGES = 2048
TEXTS = 5120
N_DP = 8


def shared_directions(key):
    feature_dir = jax.random.normal(jax.random.fold_in(key, 101), (MODEL_WIDTH,), jnp.float32)
    feature_dir = feature_dir / jnp.sqrt(jnp.sum(feature_dir * feature_dir))
    embed_dir = jax.random.normal(jax.random.fold_in(key, 102), (E,), jnp.float32)
    embed_dir = embed_dir / jnp.sqrt(jnp.sum(embed_dir * embed_dir))
    return (feature_dir, embed_dir)


def noise_draw(key, shape):
    return jax.random.normal(key, shape, jnp.float32)


def draw_resid(key, part):
    feature_dir, embed_dir = shared_directions(key)
    noise = noise_draw(jax.random.fold_in(key, 201), (IMAGES, MODEL_WIDTH))
    heavy = jax.random.uniform(jax.random.fold_in(key, 202), (IMAGES,), jnp.float32) < 0.125
    strength = jax.random.uniform(jax.random.fold_in(key, 203), (IMAGES,), jnp.float32, 3.0, 6.0)
    lift = jnp.where(heavy, strength * math.sqrt(MODEL_WIDTH), 0.0)
    rows = noise + lift[:, None] * feature_dir[None, :]
    return jnp.clip(rows, -40.0, 40.0).astype(jnp.bfloat16)


def draw_projection(key, part):
    feature_dir, embed_dir = shared_directions(key)
    base = jax.random.normal(jax.random.fold_in(key, 301), (MODEL_WIDTH, E), jnp.float32) / math.sqrt(MODEL_WIDTH)
    matrix = base + 3.0 * feature_dir[:, None] * embed_dir[None, :]
    return jnp.clip(matrix, -1.0, 1.0).astype(jnp.bfloat16)


def draw_texts(key, part):
    feature_dir, embed_dir = shared_directions(key)
    noise = noise_draw(jax.random.fold_in(key, 401), (TEXTS, E))
    order = jax.random.permutation(jax.random.fold_in(key, 402), TEXTS)
    count = max(2, TEXTS // 64)
    chosen = order[:count]
    strength = jax.random.uniform(jax.random.fold_in(key, 403), (count,), jnp.float32, 3.0, 6.0)
    rows = noise.at[chosen].add(strength[:, None] * math.sqrt(E) * embed_dir[None, :])
    return jnp.clip(rows, -48.0, 48.0).astype(jnp.bfloat16)


def with_ends(values, stream_key, least, high):
    index_at = [jax.random.randint(jax.random.fold_in(stream_key, axis), (), 0, length) for axis, length in enumerate(values.shape)]
    widest = values.shape.index(max(values.shape))
    next_to = index_at[:widest] + [(index_at[widest] + 1) % values.shape[widest]] + index_at[widest + 1:]
    return values.at[tuple(index_at)].set(least).at[tuple(next_to)].set(high)


def block_levels(key, dims, pieces, low, high):
    level, own = 1.0, jax.random.fold_in(key, 6)
    for dim, parts in pieces:
        steps = jnp.exp(jax.random.uniform(jax.random.fold_in(own, dim), (parts,), jnp.float32, low / len(pieces), high / len(pieces)))
        level = level * jnp.repeat(steps, dims[dim] // parts).reshape([-1 if axis == dim else 1 for axis in range(len(dims))])
    return level


def gaussian(rng, dims, deviation, most, pieces=(), held_as=jnp.bfloat16):
    level = block_levels(rng, dims, pieces, -0.22, 0.18) if pieces else 1.0
    values = jax.random.normal(rng, dims, jnp.float32) * deviation * level
    return jnp.minimum(jnp.maximum(values, -most), most).astype(held_as)


def setup_inputs(seed: int = 0) -> dict:
    splits = jax.random.split(jax.random.key(seed), 14)
    return {
        "resid": draw_resid(jax.random.fold_in(splits[13], 71), 0),
        "prenorm_gain": jnp.clip(1.0 + 0.15 * jax.random.normal(splits[1], (MODEL_WIDTH,), jnp.float32), 0.25, 1.75),
        "prenorm_bias": gaussian(splits[2], (MODEL_WIDTH,), 0.5, 3.0, (), jnp.float32),
        "up_weight": gaussian(splits[3], (MODEL_WIDTH, FF), MODEL_WIDTH ** -0.5, 0.1875, ((0, 8), (1, 4))),
        "up_bias": gaussian(splits[4], (FF,), 0.5, 3.0, ((0, 4),), jnp.float32),
        "down_weight": gaussian(splits[5], (FF, MODEL_WIDTH), FF ** -0.5, 0.09375, ((0, 4), (1, 8))),
        "down_bias": gaussian(splits[6], (MODEL_WIDTH,), 0.5, 3.0, (), jnp.float32),
        "post_gain": jnp.clip(1.0 + 0.15 * jax.random.normal(splits[7], (MODEL_WIDTH,), jnp.float32), 0.25, 1.75),
        "post_bias": gaussian(splits[8], (MODEL_WIDTH,), 0.5, 3.0, ((0, 4),), jnp.float32),
        "projection": draw_projection(jax.random.fold_in(splits[13], 71), 0),
        "texts": draw_texts(jax.random.fold_in(splits[13], 71), 0),
        "labels": with_ends(jax.random.randint(splits[11], (IMAGES,), 0, TEXTS), jax.random.fold_in(splits[11], 1), 0, TEXTS - 1).astype(jnp.int32),
        "step_size": jnp.clip(jnp.exp(jax.random.uniform(splits[12], (1,), jnp.float32, math.log(0.5), math.log(2.0))), 0.5, 2.0),
    }


def row_statistics(values):
    mean_val = lax.optimization_barrier(jnp.mean(values, axis=1, keepdims=True))
    var_val = lax.optimization_barrier(jnp.mean(values * values, axis=1, keepdims=True)) - mean_val * mean_val
    rstd_val = lax.rsqrt(var_val + 1e-05)
    return ((values - mean_val) * rstd_val, rstd_val)

def norm_backward_pass(grad_in, gain, normed_val, rstd_val):
    scaled = grad_in * gain
    first = lax.optimization_barrier(jnp.mean(scaled, axis=1, keepdims=True))
    second = lax.optimization_barrier(jnp.mean(scaled * normed_val, axis=1, keepdims=True))
    return (scaled - first - normed_val * second) * rstd_val

def reference(resid, prenorm_gain, prenorm_bias, up_weight, up_bias, down_weight, down_bias, post_gain, post_bias, projection, texts, labels, step_size):
    input_rows = resid.astype(jnp.float32)
    centered_input, input_inverse_deviation = row_statistics(input_rows)
    normed_input = (centered_input * prenorm_gain + prenorm_bias).astype(jnp.bfloat16)
    pre_act = jnp.dot(normed_input, up_weight, preferred_element_type=jnp.float32) + up_bias
    gate_sig = jax.nn.sigmoid(1.702 * pre_act)
    hidden = (pre_act * gate_sig).astype(jnp.bfloat16)
    block_out = input_rows + jnp.dot(hidden, down_weight, preferred_element_type=jnp.float32) + down_bias
    yhat, rstd_out = row_statistics(block_out)
    post_normed = (yhat * post_gain + post_bias).astype(jnp.bfloat16)
    embedding = jnp.dot(post_normed, projection, preferred_element_type=jnp.float32)
    emb_norm = jnp.sqrt(lax.optimization_barrier(jnp.sum(embedding * embedding, axis=1, keepdims=True)) + 1e-06)
    unit_vec = embedding / emb_norm
    unit_low = unit_vec.astype(jnp.bfloat16)
    text_f = texts.astype(jnp.float32)
    text_unit = (text_f / jnp.sqrt(lax.optimization_barrier(jnp.sum(text_f * text_f, axis=1, keepdims=True)) + 1e-06)).astype(jnp.bfloat16)

    def block_grad(pair):
        unit_blk, label_blk = pair
        logits = 100.0 * jnp.dot(unit_blk, text_unit.T, preferred_element_type=jnp.float32)
        top_val = lax.optimization_barrier(jnp.max(logits, axis=1, keepdims=True))
        exponent = jnp.exp(logits - top_val)
        prob = exponent / lax.optimization_barrier(jnp.sum(exponent, axis=1, keepdims=True))
        columns = lax.broadcasted_iota(jnp.int32, logits.shape, 1)
        target = (columns == label_blk[:, None]).astype(jnp.float32)
        score_grad = (100.0 * (prob - target)).astype(jnp.bfloat16)
        return jnp.dot(score_grad, text_unit, preferred_element_type=jnp.float32)
    unit_grad = lax.map(block_grad, (unit_low.reshape(N_DP, IMG_DEV, E), labels.astype(jnp.int32).reshape(N_DP, IMG_DEV)))
    unit_grad = unit_grad.reshape(IMAGES, E)
    along = lax.optimization_barrier(jnp.sum(unit_vec * unit_grad, axis=1, keepdims=True))
    emb_grad = ((unit_grad - unit_vec * along) / emb_norm).astype(jnp.bfloat16)
    post_grad = jnp.dot(emb_grad, projection.T, preferred_element_type=jnp.float32)
    output_gradient = norm_backward_pass(post_grad, post_gain, yhat, rstd_out)
    out_low = output_gradient.astype(jnp.bfloat16)
    hid_grad = jnp.dot(out_low, down_weight.T, preferred_element_type=jnp.float32)
    act_grad = (hid_grad * (gate_sig + 1.702 * pre_act * gate_sig * (1.0 - gate_sig))).astype(jnp.bfloat16)
    normed_gradient = jnp.dot(act_grad, up_weight.T, preferred_element_type=jnp.float32)
    input_gradient = output_gradient + norm_backward_pass(normed_gradient, prenorm_gain, centered_input, input_inverse_deviation)
    grad_rms = jnp.sqrt(lax.optimization_barrier(jnp.mean(input_gradient * input_gradient, axis=1, keepdims=True)) + 1e-06)
    return input_rows + step_size[0] * input_gradient / grad_rms
```

```python
import functools
import jax
import jax.numpy as jnp
from jax import lax
from jax.experimental import pallas as pl
from jax.experimental.pallas import tpu as pltpu
from jax.sharding import PartitionSpec as P

MESH = pl.DeviceIdType.MESH
F32 = jnp.float32
BF16 = jnp.bfloat16
RESID, PROJ, GAINS, MIXED, UNIT, STATS, BACK, OUTLOW, NORMED, FINAL = range(10)


def nn(a, b):
    return jnp.dot(a, b, preferred_element_type=F32)


def nt_dot(a, b):
    return lax.dot_general(a, b, (((1,), (1,)), ((), ())), preferred_element_type=F32)


def tiles(size, most):
    step = most if size % most == 0 else size
    return size // step, step


def kernel(
    nd, nt,
    resid, pre_gain, pre_bias, up, up_bias, down, down_bias, post_gain, post_bias,
    projection, texts, labels, step_size,
    out,
    rg, xf, normed, wu, wd, wdf, gb_s, gb, gains, pj, tu,
    hidden, dgate, part, ms, mr, us, ug, lg, sg, st_s, st, bpart, bs, br,
    os_, og, ag, ns, nr, ds_, dr,
    send, recv, ring_send, ring_recv,
):
    R, F = resid.shape
    D = nt * F
    Kd, H = up.shape
    E = projection.shape[1]
    T = texts.shape[0]
    r = R // nt
    half = nd // 2
    me = lax.axis_index("txt")
    dpi = lax.axis_index("dp")
    zz = dpi // 2
    xx = dpi % 2
    pos = zz + xx * (nd - 1 - 2 * zz)

    def at_pos(p):
        p = (p + 2 * nd) % nd
        h = p // half
        return 2 * (p + h * (nd - 1 - 2 * p)) + h

    right, left = at_pos(pos + 1), at_pos(pos - 1)

    barrier = pltpu.get_barrier_semaphore()
    for o in range(1, nt):
        pl.semaphore_signal(barrier, inc=1, device_id={"txt": (me + o) % nt}, device_id_type=MESH)
    for nb in (left, right):
        pl.semaphore_signal(barrier, inc=1, device_id={"dp": nb}, device_id_type=MESH)
    pl.semaphore_wait(barrier, nt + 1)

    def tx(which, o, src, dst):
        return pltpu.make_async_remote_copy(
            src_ref=src, dst_ref=dst, send_sem=send.at[which, o - 1], recv_sem=recv.at[which, o - 1],
            device_id={"txt": (me + o) % nt}, device_id_type=MESH)

    def exchange(which, src_of, dst):
        cs = [tx(which, o, src_of((me + o) % nt), dst) for o in range(1, nt)]
        for c in cs:
            c.start()
        return cs

    def finish(cs):
        for c in cs:
            c.wait()

    rows_of = lambda p: pl.ds(pl.multiple_of(p * r, r), r)
    mine = rows_of(me)

    def ring(kind, way, k):
        origin = at_pos(pos - k) if way == 0 else at_pos(pos + k)
        size = Kd if kind == 0 else H
        lo, n = (0, size) if k < half - 1 else ((0, size // 2) if way == 0 else (size // 2, size // 2))
        if kind == 0:
            dst = wu.at[pl.ds(pl.multiple_of(origin * Kd + lo, Kd // 2), n), :]
            src = up.at[pl.ds(lo, n), :] if k == 0 else dst
        else:
            dst = wd.at[origin, pl.ds(lo, n), :]
            src = down.at[pl.ds(lo, n), :] if k == 0 else dst
        return pltpu.make_async_remote_copy(
            src_ref=src, dst_ref=dst, send_sem=ring_send.at[kind, way, k], recv_sem=ring_recv.at[kind, way, k],
            device_id={"dp": right if way == 0 else left}, device_id_type=MESH)

    for kind in range(2):
        for way in range(2):
            ring(kind, way, 0).start()
    c_resid = exchange(RESID, lambda p: resid, rg.at[me])
    gb_s[...] = jnp.zeros_like(gb_s)
    gb_s[0:1, :] = post_gain[...]
    gb_s[1:2, :] = post_bias[...]
    c_gains = exchange(GAINS, lambda p: gb_s, gb.at[me])
    prow = pl.ds(pl.multiple_of(me * F, F), F)
    c_proj = exchange(PROJ, lambda p: projection, pj.at[prow, :])
    rg[me] = resid[...]
    gb[me] = gb_s[...]
    pj[prow, :] = projection[...]
    wu[pl.ds(pl.multiple_of(dpi * Kd, Kd), Kd), :] = up[...]

    def place(s):
        if Kd % 128 == 0:
            wdf[:, pl.ds(pl.multiple_of(s * Kd, Kd), Kd)] = wd[s]

    wd[dpi] = down[...]
    place(dpi)

    tn, tstep = tiles(T, 64)

    @pl.loop(0, tn)
    def _(i):
        sl = pl.ds(pl.multiple_of(i * tstep, tstep), tstep)
        t = texts[sl, :].astype(F32)
        tu[sl, :] = (t / jnp.sqrt(jnp.sum(t * t, axis=1, keepdims=True) + 1e-06)).astype(BF16)

    finish(c_resid)
    for t in range(nt):
        xf[:, t * F:(t + 1) * F] = rg[t].astype(F32)

    def norm_in(x):
        mean = jnp.mean(x, axis=1, keepdims=True)
        var = jnp.mean(x * x, axis=1, keepdims=True) - mean * mean
        rstd = lax.rsqrt(var + 1e-05)
        return (x - mean) * rstd, rstd

    ln, lstep = tiles(R, 64)

    @pl.loop(0, ln)
    def _(i):
        sl = pl.ds(pl.multiple_of(i * lstep, lstep), lstep)
        xhat, _ = norm_in(xf[sl, :])
        normed[sl, :] = (xhat * pre_gain[...] + pre_bias[...]).astype(BF16)

    for k in range(half):
        for kind in range(2):
            if k == half - 1 and kind == 1:
                hn, hstep = tiles(H, 256)

                @pl.loop(0, hn)
                def _(i):
                    sl = pl.ds(pl.multiple_of(i * hstep, hstep), hstep)
                    pre = nn(normed[...], wu[:, sl]) + up_bias[:, sl]
                    sig = jax.nn.sigmoid(1.702 * pre)
                    hidden[:, sl] = (pre * sig).astype(BF16)
                    dgate[:, sl] = sig + 1.702 * pre * sig * (1.0 - sig)

            for way in range(2):
                ring(kind, way, k).wait_recv()
                if k + 1 < half:
                    ring(kind, way, k + 1).start()
            if kind == 1:
                if k < half - 1:
                    place(at_pos(pos - 1 - k))
                    place(at_pos(pos + 1 + k))
                else:
                    place(at_pos(pos + half))
    if Kd % 128 != 0:
        for s in range(nd):
            wdf[:, s * Kd:(s + 1) * Kd] = wd[s]
    for k in range(half):
        for kind in range(2):
            for way in range(2):
                ring(kind, way, k).wait_send()

    dn, dstep = tiles(D, 256)

    @pl.loop(0, dn)
    def _(i):
        sl = pl.ds(pl.multiple_of(i * dstep, dstep), dstep)
        v = nn(hidden[...], wdf[:, sl])
        part[:, sl] = v
        ms[:, sl] = v.astype(BF16)

    c_mixed = exchange(MIXED, lambda p: ms.at[rows_of(p), :], mr.at[me])
    finish(c_gains)
    for t in range(nt):
        gains[:, t * F:(t + 1) * F] = gb[t]
    x_own = xf[mine, :]
    xhat_own, rstd_in = norm_in(x_own)
    block = x_own + down_bias[...] + part[mine, :]
    finish(c_mixed)
    for o in range(1, nt):
        block = block + mr[(me + o) % nt].astype(F32)
    yhat, rstd_out = norm_in(block)
    post_normed = (yhat * gains[0:1, :] + gains[1:2, :]).astype(BF16)
    finish(c_proj)
    emb = nn(post_normed, pj[...])
    emb_norm = jnp.sqrt(jnp.sum(emb * emb, axis=1, keepdims=True) + 1e-06)
    unit = emb / emb_norm
    us[...] = unit.astype(BF16)
    c_unit = exchange(UNIT, lambda p: us, ug.at[mine, :])
    ug[mine, :] = us[...]
    finish(c_unit)

    kn, kstep = tiles(T, 256)

    def logit_tile(i, m):
        sl = pl.ds(pl.multiple_of(i * kstep, kstep), kstep)
        l = 100.0 * nt_dot(ug[...], tu[sl, :])
        lg[:, sl] = l
        return jnp.maximum(m, jnp.max(l, axis=1, keepdims=True))

    top = lax.fori_loop(0, kn, logit_tile, jnp.full((R, 1), -jnp.inf, F32))

    def exp_tile(i, s):
        sl = pl.ds(pl.multiple_of(i * kstep, kstep), kstep)
        e = jnp.exp(lg[:, sl] - top)
        lg[:, sl] = e
        return s + jnp.sum(e, axis=1, keepdims=True)

    total = lax.fori_loop(0, kn, exp_tile, jnp.zeros((R, 1), F32))
    lane = lax.broadcasted_iota(jnp.int32, (R, 128), 1)
    packed = jnp.where(lane == 0, top, total)
    st_s[...] = packed.T[0:8, :]
    c_stats = exchange(STATS, lambda p: st_s, st.at[me])
    st[me] = st_s[...]
    finish(c_stats)
    allm = st[0, 0:1, :]
    for t in range(1, nt):
        allm = jnp.maximum(allm, st[t, 0:1, :])
    alls = jnp.zeros_like(allm)
    for t in range(nt):
        alls = alls + st[t, 1:2, :] * jnp.exp(st[t, 0:1, :] - allm)
    row = lax.broadcasted_iota(jnp.int32, (128, R), 0)
    back_t = jnp.where(row == 0, allm, alls).T
    factor = jnp.exp(top - back_t[:, 0:1]) / back_t[:, 1:2]
    local_label = labels[...] - me * T

    @pl.loop(0, kn)
    def _(i):
        sl = pl.ds(pl.multiple_of(i * kstep, kstep), kstep)
        prob = lg[:, sl] * factor
        cols = lax.broadcasted_iota(jnp.int32, (R, kstep), 1) + i * kstep
        target = (cols == local_label).astype(F32)
        sg[:, sl] = (100.0 * (prob - target)).astype(BF16)

    en, estep = tiles(E, 256)

    @pl.loop(0, en)
    def _(i):
        sl = pl.ds(pl.multiple_of(i * estep, estep), estep)
        v = nn(sg[...], tu[:, sl])
        bpart[:, sl] = v
        bs[:, sl] = v.astype(BF16)

    c_back = exchange(BACK, lambda p: bs.at[rows_of(p), :], br.at[me])
    ugrad = bpart[mine, :]
    finish(c_back)
    for o in range(1, nt):
        ugrad = ugrad + br[(me + o) % nt].astype(F32)
    along = jnp.sum(unit * ugrad, axis=1, keepdims=True)
    emb_grad = ((ugrad - unit * along) / emb_norm).astype(BF16)

    def norm_back(scaled, hat, rstd):
        first = jnp.mean(scaled, axis=1, keepdims=True)
        second = jnp.mean(scaled * hat, axis=1, keepdims=True)
        return (scaled - first - hat * second) * rstd

    out_grad = norm_back(nt_dot(emb_grad, pj[...]) * gains[0:1, :], yhat, rstd_out)
    os_[...] = out_grad.astype(BF16)
    c_out = exchange(OUTLOW, lambda p: os_, og.at[mine, :])
    og[mine, :] = os_[...]
    finish(c_out)
    hn, hstep = tiles(H, 256)

    @pl.loop(0, hn)
    def _(i):
        sl = pl.ds(pl.multiple_of(i * hstep, hstep), hstep)
        ag[:, sl] = (nt_dot(og[...], wdf[sl, :]) * dgate[:, sl]).astype(BF16)

    @pl.loop(0, dn)
    def _(i):
        sl = pl.ds(pl.multiple_of(i * dstep, dstep), dstep)
        v = nt_dot(ag[...], wu[sl, :])
        part[:, sl] = v
        ns[:, sl] = v.astype(BF16)

    c_norm = exchange(NORMED, lambda p: ns.at[rows_of(p), :], nr.at[me])
    ngrad = part[mine, :]
    finish(c_norm)
    for o in range(1, nt):
        ngrad = ngrad + nr[(me + o) % nt].astype(F32)
    in_grad = out_grad + norm_back(ngrad * pre_gain[...], xhat_own, rstd_in)
    rms = jnp.sqrt(jnp.mean(in_grad * in_grad, axis=1, keepdims=True) + 1e-06)
    delta = step_size[0] * in_grad / rms
    for t in range(nt):
        ds_[t] = delta[:, t * F:(t + 1) * F]
    c_fin = exchange(FINAL, lambda p: ds_.at[p], dr.at[mine, :])
    dr[mine, :] = ds_[me]
    finish(c_fin)
    out[...] = resid[...].astype(F32) + dr[...]


def solution(mesh):
    nd, nt = mesh.shape["dp"], mesh.shape["txt"]
    placed = (
        P("dp", "txt"),
        P(),
        P(),
        P("dp", "txt"),
        P("txt"),
        P("txt", "dp"),
        P(),
        P("txt"),
        P("txt"),
        P("txt", None),
        P("txt", None),
        P("dp"),
        P(),
    )

    def local(resid, pre_gain, pre_bias, up, up_bias, down, down_bias, post_gain, post_bias,
              projection, texts, labels, step_size):
        R, F = resid.shape
        D = nt * F
        Kd, H = up.shape
        E = projection.shape[1]
        T = texts.shape[0]
        r = R // nt
        V = pltpu.VMEM
        scratch = [
            V((nt, R, F), BF16),
            V((R, D), F32),
            V((R, D), BF16),
            V((D, H), BF16),
            V((nd, H, Kd), BF16),
            V((H, D), BF16),
            V((8, F), F32),
            V((nt, 8, F), F32),
            V((8, D), F32),
            V((D, E), BF16),
            V((T, E), BF16),
            V((R, H), BF16),
            V((R, H), F32),
            V((R, D), F32),
            V((R, D), BF16),
            V((nt, r, D), BF16),
            V((r, E), BF16),
            V((R, E), BF16),
            V((R, T), F32),
            V((R, T), BF16),
            V((8, R), F32),
            V((nt, 8, R), F32),
            V((R, E), F32),
            V((R, E), BF16),
            V((nt, r, E), BF16),
            V((r, D), BF16),
            V((R, D), BF16),
            V((R, H), BF16),
            V((R, D), BF16),
            V((nt, r, D), BF16),
            V((nt, r, F), F32),
            V((R, F), F32),
            pltpu.SemaphoreType.DMA((10, nt - 1)),
            pltpu.SemaphoreType.DMA((10, nt - 1)),
            pltpu.SemaphoreType.DMA((2, 2, nd // 2)),
            pltpu.SemaphoreType.DMA((2, 2, nd // 2)),
        ]
        vm = pl.BlockSpec(memory_space=pltpu.VMEM)
        line = lambda v: v.reshape(1, -1)
        return pl.pallas_call(
            functools.partial(kernel, nd, nt),
            out_shape=jax.ShapeDtypeStruct((R, F), F32),
            in_specs=[vm] * 12 + [pl.BlockSpec(memory_space=pltpu.SMEM)],
            out_specs=vm,
            scratch_shapes=scratch,
            compiler_params=pltpu.CompilerParams(
                collective_id=0, has_side_effects=True, vmem_limit_bytes=60 * 1024 * 1024),
        )(resid, line(pre_gain), line(pre_bias), up, line(up_bias), down, line(down_bias),
          line(post_gain), line(post_bias), projection, texts, labels.reshape(-1, 1), step_size)

    return jax.shard_map(local, mesh=mesh, in_specs=placed, out_specs=P("dp", "txt"), check_vma=False)
```

```python
import functools
import jax
import jax.numpy as jnp
from jax import lax
from jax.experimental import pallas as pl
from jax.experimental.pallas import tpu as pltpu
from jax.sharding import PartitionSpec as P

MESH = pl.DeviceIdType.MESH
F32 = jnp.float32
BF16 = jnp.bfloat16
RESID, PROJ, GAINS, MIXED, UNIT, STATS, BACK, OUTLOW, NORMED, FINAL = range(10)


def nn(a, b):
    return jnp.dot(a, b, preferred_element_type=F32)


def nt_dot(a, b):
    return lax.dot_general(a, b, (((1,), (1,)), ((), ())), preferred_element_type=F32)


def tiles(size, most):
    step = most if size % most == 0 else size
    return size // step, step


def halves(r):
    return 2 if r % 32 == 0 else 1


def kernel(
    nd, nt,
    resid, pre_gain, pre_bias, up, up_bias, down, down_bias, post_gain, post_bias,
    projection, texts, labels, step_size,
    out,
    rg, xf, normed, wu, wd, wdf, gb_s, gb, gains, pj, tu,
    hidden, dgate, part, ms, mr, us, ug, lg, sg, st_s, st, bpart, bs, br,
    os_, og, ag, ns, nr, ds_, dr,
    lab, traw, text_sem, send, recv, ring_send, ring_recv,
):
    R, F = resid.shape
    D = nt * F
    Kd, H = up.shape
    E = projection.shape[1]
    T = texts.shape[0]
    r = R // nt
    NH = halves(r)
    rh, Rh = r // NH, R // NH
    half = nd // 2
    me = lax.axis_index("txt")
    dpi = lax.axis_index("dp")
    zz = dpi // 2
    xx = dpi % 2
    pos = zz + xx * (nd - 1 - 2 * zz)

    def at_pos(p):
        p = (p + 2 * nd) % nd
        h = p // half
        return 2 * (p + h * (nd - 1 - 2 * p)) + h

    right, left = at_pos(pos + 1), at_pos(pos - 1)

    text_copy = pltpu.make_async_copy(texts, traw, text_sem)
    text_copy.start()
    barrier = pltpu.get_barrier_semaphore()
    for o in range(1, nt):
        pl.semaphore_signal(barrier, inc=1, device_id={"txt": (me + o) % nt}, device_id_type=MESH)
    for nb in (left, right):
        pl.semaphore_signal(barrier, inc=1, device_id={"dp": nb}, device_id_type=MESH)
    pl.semaphore_wait(barrier, nt + 1)

    def tx(which, h, o, src, dst):
        return pltpu.make_async_remote_copy(
            src_ref=src, dst_ref=dst, send_sem=send.at[h, which, o - 1], recv_sem=recv.at[h, which, o - 1],
            device_id={"txt": (me + o) % nt}, device_id_type=MESH)

    def exchange(which, src_of, dst, h=0):
        cs = [tx(which, h, o, src_of((me + o) % nt), dst) for o in range(1, nt)]
        for c in cs:
            c.start()
        return cs

    def finish(cs):
        for c in cs:
            c.wait()

    in_half = lambda p: pl.ds(pl.multiple_of(p * rh, rh), rh)
    rows_of = lambda h, p: pl.ds(pl.multiple_of(h * Rh + p * rh, rh), rh)
    whole_half = lambda h: pl.ds(h * Rh, Rh)

    def ring(kind, way, k):
        origin = at_pos(pos - k) if way == 0 else at_pos(pos + k)
        size = Kd if kind == 0 else H
        lo, n = (0, size) if k < half - 1 else ((0, size // 2) if way == 0 else (size // 2, size // 2))
        if kind == 0:
            dst = wu.at[pl.ds(pl.multiple_of(origin * Kd + lo, Kd // 2), n), :]
            src = up.at[pl.ds(lo, n), :] if k == 0 else dst
        else:
            dst = wd.at[origin, pl.ds(lo, n), :]
            src = down.at[pl.ds(lo, n), :] if k == 0 else dst
        return pltpu.make_async_remote_copy(
            src_ref=src, dst_ref=dst, send_sem=ring_send.at[kind, way, k], recv_sem=ring_recv.at[kind, way, k],
            device_id={"dp": right if way == 0 else left}, device_id_type=MESH)

    for kind in range(2):
        for way in range(2):
            ring(kind, way, 0).start()
    c_resid = exchange(RESID, lambda p: resid, rg.at[me])
    gb_s[...] = jnp.zeros_like(gb_s)
    gb_s[0:1, :] = post_gain[...]
    gb_s[1:2, :] = post_bias[...]
    c_gains = exchange(GAINS, lambda p: gb_s, gb.at[me])
    prow = pl.ds(pl.multiple_of(me * F, F), F)
    c_proj = exchange(PROJ, lambda p: projection, pj.at[prow, :])
    rg[me] = resid[...]
    gb[me] = gb_s[...]
    pj[prow, :] = projection[...]
    wu[pl.ds(pl.multiple_of(dpi * Kd, Kd), Kd), :] = up[...]

    def place(s):
        if Kd % 128 == 0:
            wdf[:, pl.ds(pl.multiple_of(s * Kd, Kd), Kd)] = wd[s]

    wd[dpi] = down[...]
    place(dpi)

    lab_t = jnp.broadcast_to(labels[...].astype(F32), (128, R)).T
    for h in range(NH):
        for p in range(nt):
            q, n = h * Rh + p * rh, p * r + h * rh
            lab[q:q + rh, :] = lab_t[n:n + rh, :]

    text_copy.wait()
    tn, tstep = tiles(T, 64)

    @pl.loop(0, tn)
    def _(i):
        sl = pl.ds(pl.multiple_of(i * tstep, tstep), tstep)
        t = traw[sl, :].astype(F32)
        tu[sl, :] = (t / jnp.sqrt(jnp.sum(t * t, axis=1, keepdims=True) + 1e-06)).astype(BF16)

    finish(c_resid)
    for t in range(nt):
        for h in range(NH):
            for p in range(nt):
                q, n = h * Rh + p * rh, p * r + h * rh
                xf[q:q + rh, t * F:(t + 1) * F] = rg[t, n:n + rh, :].astype(F32)

    def norm_in(x):
        mean = jnp.mean(x, axis=1, keepdims=True)
        var = jnp.mean(x * x, axis=1, keepdims=True) - mean * mean
        rstd = lax.rsqrt(var + 1e-05)
        return (x - mean) * rstd, rstd

    ln, lstep = tiles(R, 64)

    @pl.loop(0, ln)
    def _(i):
        sl = pl.ds(pl.multiple_of(i * lstep, lstep), lstep)
        xhat, _ = norm_in(xf[sl, :])
        normed[sl, :] = (xhat * pre_gain[...] + pre_bias[...]).astype(BF16)

    for k in range(half):
        for kind in range(2):
            if k == half - 1 and kind == 1:
                hn, hstep = tiles(H, 256)

                @pl.loop(0, hn)
                def _(i):
                    sl = pl.ds(pl.multiple_of(i * hstep, hstep), hstep)
                    pre = nn(normed[...], wu[:, sl]) + up_bias[:, sl]
                    sig = jax.nn.sigmoid(1.702 * pre)
                    hidden[:, sl] = (pre * sig).astype(BF16)
                    dgate[:, sl] = sig + 1.702 * pre * sig * (1.0 - sig)

            for way in range(2):
                ring(kind, way, k).wait_recv()
                if k + 1 < half:
                    ring(kind, way, k + 1).start()
            if kind == 1:
                if k < half - 1:
                    place(at_pos(pos - 1 - k))
                    place(at_pos(pos + 1 + k))
                else:
                    place(at_pos(pos + half))
    if Kd % 128 != 0:
        for s in range(nd):
            wdf[:, s * Kd:(s + 1) * Kd] = wd[s]
    for k in range(half):
        for kind in range(2):
            for way in range(2):
                ring(kind, way, k).wait_send()

    dn, dstep = tiles(D, 256)
    hn, hstep = tiles(H, 256)
    kn, kstep = tiles(T, 256)
    en, estep = tiles(E, 256)
    both = range(NH)
    c_mixed, c_unit, c_stats, c_back, c_out, c_norm, c_fin = ([None] * NH for _ in range(7))
    xhat_own, rstd_in, yhat, rstd_out, unit, emb_norm, out_grad, tops = ([None] * NH for _ in range(8))

    def norm_back(scaled, hat, rstd):
        first = jnp.mean(scaled, axis=1, keepdims=True)
        second = jnp.mean(scaled * hat, axis=1, keepdims=True)
        return (scaled - first - hat * second) * rstd

    for h in both:
        hs = whole_half(h)

        @pl.loop(0, dn)
        def _(i):
            sl = pl.ds(pl.multiple_of(i * dstep, dstep), dstep)
            v = nn(hidden[hs, :], wdf[:, sl])
            part[hs, sl] = v
            ms[hs, sl] = v.astype(BF16)

        c_mixed[h] = exchange(MIXED, lambda p: ms.at[rows_of(h, p), :], mr.at[h, me], h)

    finish(c_gains)
    for t in range(nt):
        gains[:, t * F:(t + 1) * F] = gb[t]

    for h in both:
        own = rows_of(h, me)
        x_own = xf[own, :]
        xhat_own[h], rstd_in[h] = norm_in(x_own)
        block = x_own + down_bias[...] + part[own, :]
        finish(c_mixed[h])
        for o in range(1, nt):
            block = block + mr[h, (me + o) % nt].astype(F32)
        yhat[h], rstd_out[h] = norm_in(block)
        post_normed = (yhat[h] * gains[0:1, :] + gains[1:2, :]).astype(BF16)
        if h == 0:
            finish(c_proj)
        emb = nn(post_normed, pj[...])
        emb_norm[h] = jnp.sqrt(jnp.sum(emb * emb, axis=1, keepdims=True) + 1e-06)
        unit[h] = emb / emb_norm[h]
        us[h] = unit[h].astype(BF16)
        c_unit[h] = exchange(UNIT, lambda p: us.at[h], ug.at[own, :], h)
        ug[own, :] = us[h]

    for h in both:
        hs = whole_half(h)
        finish(c_unit[h])

        def logit_tile(i, m):
            sl = pl.ds(pl.multiple_of(i * kstep, kstep), kstep)
            l = 100.0 * nt_dot(ug[hs, :], tu[sl, :])
            lg[hs, sl] = l
            return jnp.maximum(m, jnp.max(l, axis=1, keepdims=True))

        top = lax.fori_loop(0, kn, logit_tile, jnp.full((Rh, 1), -jnp.inf, F32))

        def exp_tile(i, s):
            sl = pl.ds(pl.multiple_of(i * kstep, kstep), kstep)
            e = jnp.exp(lg[hs, sl] - top)
            lg[hs, sl] = e
            return s + jnp.sum(e, axis=1, keepdims=True)

        total = lax.fori_loop(0, kn, exp_tile, jnp.zeros((Rh, 1), F32))
        tops[h] = top
        lane = lax.broadcasted_iota(jnp.int32, (Rh, 128), 1)
        st_s[h] = jnp.where(lane == 0, top, total).T[0:8, :]
        c_stats[h] = exchange(STATS, lambda p: st_s.at[h], st.at[h, me], h)
        st[h, me] = st_s[h]

    for h in both:
        hs = whole_half(h)
        local_label = lab[hs, 0:1] - (me * T).astype(F32)
        finish(c_stats[h])
        allm = st[h, 0, 0:1, :]
        for t in range(1, nt):
            allm = jnp.maximum(allm, st[h, t, 0:1, :])
        alls = jnp.zeros_like(allm)
        for t in range(nt):
            alls = alls + st[h, t, 1:2, :] * jnp.exp(st[h, t, 0:1, :] - allm)
        row = lax.broadcasted_iota(jnp.int32, (128, Rh), 0)
        back_t = jnp.where(row == 0, allm, alls).T
        factor = jnp.exp(tops[h] - back_t[:, 0:1]) / back_t[:, 1:2]

        @pl.loop(0, kn)
        def _(i):
            sl = pl.ds(pl.multiple_of(i * kstep, kstep), kstep)
            prob = lg[hs, sl] * factor
            cols = (lax.broadcasted_iota(jnp.int32, (Rh, kstep), 1) + i * kstep).astype(F32)
            target = (cols == local_label).astype(F32)
            sg[hs, sl] = (100.0 * (prob - target)).astype(BF16)

        @pl.loop(0, en)
        def _(i):
            sl = pl.ds(pl.multiple_of(i * estep, estep), estep)
            v = nn(sg[hs, :], tu[:, sl])
            bpart[hs, sl] = v
            bs[hs, sl] = v.astype(BF16)

        c_back[h] = exchange(BACK, lambda p: bs.at[rows_of(h, p), :], br.at[h, me], h)

    for h in both:
        own = rows_of(h, me)
        ugrad = bpart[own, :]
        finish(c_back[h])
        for o in range(1, nt):
            ugrad = ugrad + br[h, (me + o) % nt].astype(F32)
        along = jnp.sum(unit[h] * ugrad, axis=1, keepdims=True)
        emb_grad = ((ugrad - unit[h] * along) / emb_norm[h]).astype(BF16)
        out_grad[h] = norm_back(nt_dot(emb_grad, pj[...]) * gains[0:1, :], yhat[h], rstd_out[h])
        os_[h] = out_grad[h].astype(BF16)
        c_out[h] = exchange(OUTLOW, lambda p: os_.at[h], og.at[own, :], h)
        og[own, :] = os_[h]

    for h in both:
        hs = whole_half(h)
        finish(c_out[h])

        @pl.loop(0, hn)
        def _(i):
            sl = pl.ds(pl.multiple_of(i * hstep, hstep), hstep)
            ag[hs, sl] = (nt_dot(og[hs, :], wdf[sl, :]) * dgate[hs, sl]).astype(BF16)

        @pl.loop(0, dn)
        def _(i):
            sl = pl.ds(pl.multiple_of(i * dstep, dstep), dstep)
            v = nt_dot(ag[hs, :], wu[sl, :])
            part[hs, sl] = v
            ns[hs, sl] = v.astype(BF16)

        c_norm[h] = exchange(NORMED, lambda p: ns.at[rows_of(h, p), :], nr.at[h, me], h)

    for h in both:
        ngrad = part[rows_of(h, me), :]
        finish(c_norm[h])
        for o in range(1, nt):
            ngrad = ngrad + nr[h, (me + o) % nt].astype(F32)
        in_grad = out_grad[h] + norm_back(ngrad * pre_gain[...], xhat_own[h], rstd_in[h])
        rms = jnp.sqrt(jnp.mean(in_grad * in_grad, axis=1, keepdims=True) + 1e-06)
        delta = step_size[0] * in_grad / rms
        for t in range(nt):
            ds_[h, t] = delta[:, t * F:(t + 1) * F]
        land = pl.ds(pl.multiple_of(me * r + h * rh, rh), rh)
        c_fin[h] = exchange(FINAL, lambda p: ds_.at[h, p], dr.at[land, :], h)
        dr[land, :] = ds_[h, me]
    for h in both:
        finish(c_fin[h])
    out[...] = resid[...].astype(F32) + dr[...]


def solution(mesh):
    nd, nt = mesh.shape["dp"], mesh.shape["txt"]
    placed = (
        P("dp", "txt"),
        P(),
        P(),
        P("dp", "txt"),
        P("txt"),
        P("txt", "dp"),
        P(),
        P("txt"),
        P("txt"),
        P("txt", None),
        P("txt", None),
        P("dp"),
        P(),
    )

    def local(resid, pre_gain, pre_bias, up, up_bias, down, down_bias, post_gain, post_bias,
              projection, texts, labels, step_size):
        R, F = resid.shape
        D = nt * F
        Kd, H = up.shape
        E = projection.shape[1]
        T = texts.shape[0]
        r = R // nt
        NH = halves(r)
        rh, Rh = r // NH, R // NH
        V = pltpu.VMEM
        scratch = [
            V((nt, R, F), BF16),
            V((R, D), F32),
            V((R, D), BF16),
            V((D, H), BF16),
            V((nd, H, Kd), BF16),
            V((H, D), BF16),
            V((8, F), F32),
            V((nt, 8, F), F32),
            V((8, D), F32),
            V((D, E), BF16),
            V((T, E), BF16),
            V((R, H), BF16),
            V((R, H), F32),
            V((R, D), F32),
            V((R, D), BF16),
            V((NH, nt, rh, D), BF16),
            V((NH, rh, E), BF16),
            V((R, E), BF16),
            V((R, T), F32),
            V((R, T), BF16),
            V((NH, 8, Rh), F32),
            V((NH, nt, 8, Rh), F32),
            V((R, E), F32),
            V((R, E), BF16),
            V((NH, nt, rh, E), BF16),
            V((NH, rh, D), BF16),
            V((R, D), BF16),
            V((R, H), BF16),
            V((R, D), BF16),
            V((NH, nt, rh, D), BF16),
            V((NH, nt, rh, F), F32),
            V((R, F), F32),
            V((R, 128), F32),
            V((T, E), BF16),
            pltpu.SemaphoreType.DMA,
            pltpu.SemaphoreType.DMA((NH, 10, nt - 1)),
            pltpu.SemaphoreType.DMA((NH, 10, nt - 1)),
            pltpu.SemaphoreType.DMA((2, 2, nd // 2)),
            pltpu.SemaphoreType.DMA((2, 2, nd // 2)),
        ]
        vm = pl.BlockSpec(memory_space=pltpu.VMEM)
        line = lambda v: v.reshape(1, -1)
        return pl.pallas_call(
            functools.partial(kernel, nd, nt),
            out_shape=jax.ShapeDtypeStruct((R, F), F32),
            in_specs=[vm] * 10 + [pl.BlockSpec(memory_space=pl.ANY), vm] + [pl.BlockSpec(memory_space=pltpu.SMEM)],
            out_specs=vm,
            scratch_shapes=scratch,
            compiler_params=pltpu.CompilerParams(
                collective_id=0, has_side_effects=True, vmem_limit_bytes=60 * 1024 * 1024),
        )(resid, line(pre_gain), line(pre_bias), up, line(up_bias), down, line(down_bias),
          line(post_gain), line(post_bias), projection, texts, line(labels), step_size)

    return jax.shard_map(local, mesh=mesh, in_specs=placed, out_specs=P("dp", "txt"), check_vma=False)
```

```python
import functools
import jax
import jax.numpy as jnp
from jax import lax
from jax.experimental import pallas as pl
from jax.experimental.pallas import tpu as pltpu
from jax.sharding import PartitionSpec as P

MESH = pl.DeviceIdType.MESH
F32 = jnp.float32
BF16 = jnp.bfloat16
RESID, PROJ, GAINS, MIXED, UNIT, STATS, BACK, OUTLOW, NORMED, FINAL = range(10)


def nn(a, b):
    return jnp.dot(a, b, preferred_element_type=F32)


def nt_dot(a, b):
    return lax.dot_general(a, b, (((1,), (1,)), ((), ())), preferred_element_type=F32)


def tiles(size, most):
    step = most if size % most == 0 else size
    return size // step, step


def halves(r):
    return 2 if r % 32 == 0 else 1


def kernel(
    nd, nt,
    resid, pre_gain, pre_bias, up, up_bias, down, down_bias, post_gain, post_bias,
    projection, texts, labels, step_size,
    out,
    rg, xf, normed, wu, wd, wdf, gb_s, gb, gains, pj, tu,
    hidden, dgate, part, ms, mr, us, ug, lg, sg, st_s, st, bpart, bs, br,
    os_, og, ag, ns, nr, ds_, dr,
    lab, traw, text_sem, send, recv, ring_send, ring_recv,
):
    R, F = resid.shape
    D = nt * F
    Kd, H = up.shape
    E = projection.shape[1]
    T = texts.shape[0]
    r = R // nt
    NH = halves(r)
    rh, Rh = r // NH, R // NH
    half = nd // 2
    me = lax.axis_index("txt")
    dpi = lax.axis_index("dp")
    zz = dpi // 2
    xx = dpi % 2
    pos = zz + xx * (nd - 1 - 2 * zz)

    def at_pos(p):
        p = (p + 2 * nd) % nd
        h = p // half
        return 2 * (p + h * (nd - 1 - 2 * p)) + h

    right, left = at_pos(pos + 1), at_pos(pos - 1)

    text_copy = pltpu.make_async_copy(texts, traw, text_sem)
    text_copy.start()
    barrier = pltpu.get_barrier_semaphore()
    for o in range(1, nt):
        pl.semaphore_signal(barrier, inc=1, device_id={"txt": (me + o) % nt}, device_id_type=MESH)
    for nb in (left, right):
        pl.semaphore_signal(barrier, inc=1, device_id={"dp": nb}, device_id_type=MESH)
    pl.semaphore_wait(barrier, nt + 1)

    def tx(which, h, o, src, dst):
        return pltpu.make_async_remote_copy(
            src_ref=src, dst_ref=dst, send_sem=send.at[h, which, o - 1], recv_sem=recv.at[h, which, o - 1],
            device_id={"txt": (me + o) % nt}, device_id_type=MESH)

    def exchange(which, src_of, dst, h=0):
        cs = [tx(which, h, o, src_of((me + o) % nt), dst) for o in range(1, nt)]
        for c in cs:
            c.start()
        return cs

    def finish(cs):
        for c in cs:
            c.wait()

    in_half = lambda p: pl.ds(pl.multiple_of(p * rh, rh), rh)
    rows_of = lambda h, p: pl.ds(pl.multiple_of(h * Rh + p * rh, rh), rh)
    whole_half = lambda h: pl.ds(h * Rh, Rh)

    def ring(kind, way, k):
        origin = at_pos(pos - k) if way == 0 else at_pos(pos + k)
        size = Kd if kind == 0 else H
        lo, n = (0, size) if k < half - 1 else ((0, size // 2) if way == 0 else (size // 2, size // 2))
        if kind == 0:
            dst = wu.at[pl.ds(pl.multiple_of(origin * Kd + lo, Kd // 2), n), :]
            src = up.at[pl.ds(lo, n), :] if k == 0 else dst
        else:
            dst = wd.at[origin, pl.ds(lo, n), :]
            src = down.at[pl.ds(lo, n), :] if k == 0 else dst
        return pltpu.make_async_remote_copy(
            src_ref=src, dst_ref=dst, send_sem=ring_send.at[kind, way, k], recv_sem=ring_recv.at[kind, way, k],
            device_id={"dp": right if way == 0 else left}, device_id_type=MESH)

    for kind in range(2):
        for way in range(2):
            ring(kind, way, 0).start()
    c_resid = exchange(RESID, lambda p: resid, rg.at[me])
    gb_s[...] = jnp.zeros_like(gb_s)
    gb_s[0:1, :] = post_gain[...]
    gb_s[1:2, :] = post_bias[...]
    c_gains = exchange(GAINS, lambda p: gb_s, gb.at[me])
    prow = pl.ds(pl.multiple_of(me * F, F), F)
    c_proj = exchange(PROJ, lambda p: projection, pj.at[prow, :])
    rg[me] = resid[...]
    gb[me] = gb_s[...]
    pj[prow, :] = projection[...]
    wu[pl.ds(pl.multiple_of(dpi * Kd, Kd), Kd), :] = up[...]

    def place(s):
        if Kd % 128 == 0:
            wdf[:, pl.ds(pl.multiple_of(s * Kd, Kd), Kd)] = wd[s]

    wd[dpi] = down[...]
    place(dpi)

    lab_t = jnp.broadcast_to(labels[...].astype(F32), (128, R)).T
    for h in range(NH):
        for p in range(nt):
            q, n = h * Rh + p * rh, p * r + h * rh
            lab[q:q + rh, :] = lab_t[n:n + rh, :]

    text_copy.wait()
    tn, tstep = tiles(T, 64)

    @pl.loop(0, tn)
    def _(i):
        sl = pl.ds(pl.multiple_of(i * tstep, tstep), tstep)
        t = traw[sl, :].astype(F32)
        tu[sl, :] = (t / jnp.sqrt(jnp.sum(t * t, axis=1, keepdims=True) + 1e-06)).astype(BF16)

    finish(c_resid)
    for t in range(nt):
        for h in range(NH):
            for p in range(nt):
                q, n = h * Rh + p * rh, p * r + h * rh
                xf[q:q + rh, t * F:(t + 1) * F] = rg[t, n:n + rh, :].astype(F32)

    def norm_in(x):
        mean = jnp.mean(x, axis=1, keepdims=True)
        var = jnp.mean(x * x, axis=1, keepdims=True) - mean * mean
        rstd = lax.rsqrt(var + 1e-05)
        return (x - mean) * rstd, rstd

    ln, lstep = tiles(R, 64)

    @pl.loop(0, ln)
    def _(i):
        sl = pl.ds(pl.multiple_of(i * lstep, lstep), lstep)
        xhat, _ = norm_in(xf[sl, :])
        normed[sl, :] = (xhat * pre_gain[...] + pre_bias[...]).astype(BF16)

    for k in range(half):
        for kind in range(2):
            if k == half - 1 and kind == 1:
                hn, hstep = tiles(H, 256)

                @pl.loop(0, hn, unroll=True)
                def _(i):
                    sl = pl.ds(pl.multiple_of(i * hstep, hstep), hstep)
                    pre = nn(normed[...], wu[:, sl]) + up_bias[:, sl]
                    sig = jax.nn.sigmoid(1.702 * pre)
                    hidden[:, sl] = (pre * sig).astype(BF16)
                    dgate[:, sl] = sig + 1.702 * pre * sig * (1.0 - sig)

            for way in range(2):
                ring(kind, way, k).wait_recv()
                if k + 1 < half:
                    ring(kind, way, k + 1).start()
            if kind == 1:
                if k < half - 1:
                    place(at_pos(pos - 1 - k))
                    place(at_pos(pos + 1 + k))
                else:
                    place(at_pos(pos + half))
    if Kd % 128 != 0:
        for s in range(nd):
            wdf[:, s * Kd:(s + 1) * Kd] = wd[s]
    for k in range(half):
        for kind in range(2):
            for way in range(2):
                ring(kind, way, k).wait_send()

    dn, dstep = tiles(D, 256)
    hn, hstep = tiles(H, 256)
    kn, kstep = tiles(T, 256)
    en, estep = tiles(E, 256)
    both = range(NH)
    c_mixed, c_unit, c_stats, c_back, c_out, c_norm, c_fin = ([None] * NH for _ in range(7))
    xhat_own, rstd_in, yhat, rstd_out, unit, emb_norm, out_grad, tops = ([None] * NH for _ in range(8))

    def norm_back(scaled, hat, rstd):
        first = jnp.mean(scaled, axis=1, keepdims=True)
        second = jnp.mean(scaled * hat, axis=1, keepdims=True)
        return (scaled - first - hat * second) * rstd

    for h in both:
        hs = whole_half(h)

        @pl.loop(0, dn, unroll=True)
        def _(i):
            sl = pl.ds(pl.multiple_of(i * dstep, dstep), dstep)
            v = nn(hidden[hs, :], wdf[:, sl])
            part[hs, sl] = v
            ms[hs, sl] = v.astype(BF16)

        c_mixed[h] = exchange(MIXED, lambda p: ms.at[rows_of(h, p), :], mr.at[h, me], h)

    finish(c_gains)
    for t in range(nt):
        gains[:, t * F:(t + 1) * F] = gb[t]

    for h in both:
        own = rows_of(h, me)
        x_own = xf[own, :]
        xhat_own[h], rstd_in[h] = norm_in(x_own)
        block = x_own + down_bias[...] + part[own, :]
        finish(c_mixed[h])
        for o in range(1, nt):
            block = block + mr[h, (me + o) % nt].astype(F32)
        yhat[h], rstd_out[h] = norm_in(block)
        post_normed = (yhat[h] * gains[0:1, :] + gains[1:2, :]).astype(BF16)
        if h == 0:
            finish(c_proj)
        emb = nn(post_normed, pj[...])
        emb_norm[h] = jnp.sqrt(jnp.sum(emb * emb, axis=1, keepdims=True) + 1e-06)
        unit[h] = emb / emb_norm[h]
        us[h] = unit[h].astype(BF16)
        c_unit[h] = exchange(UNIT, lambda p: us.at[h], ug.at[own, :], h)
        ug[own, :] = us[h]

    for h in both:
        hs = whole_half(h)
        finish(c_unit[h])

        def logit_tile(i, m):
            sl = pl.ds(pl.multiple_of(i * kstep, kstep), kstep)
            l = 100.0 * nt_dot(ug[hs, :], tu[sl, :])
            lg[hs, sl] = l
            return jnp.maximum(m, jnp.max(l, axis=1, keepdims=True))

        top = lax.fori_loop(0, kn, logit_tile, jnp.full((Rh, 1), -jnp.inf, F32), unroll=True)

        def exp_tile(i, s):
            sl = pl.ds(pl.multiple_of(i * kstep, kstep), kstep)
            e = jnp.exp(lg[hs, sl] - top)
            lg[hs, sl] = e
            return s + jnp.sum(e, axis=1, keepdims=True)

        total = lax.fori_loop(0, kn, exp_tile, jnp.zeros((Rh, 1), F32), unroll=True)
        tops[h] = top
        lane = lax.broadcasted_iota(jnp.int32, (Rh, 128), 1)
        st_s[h] = jnp.where(lane == 0, top, total).T[0:8, :]
        c_stats[h] = exchange(STATS, lambda p: st_s.at[h], st.at[h, me], h)
        st[h, me] = st_s[h]

    for h in both:
        hs = whole_half(h)
        local_label = lab[hs, 0:1] - (me * T).astype(F32)
        finish(c_stats[h])
        allm = st[h, 0, 0:1, :]
        for t in range(1, nt):
            allm = jnp.maximum(allm, st[h, t, 0:1, :])
        alls = jnp.zeros_like(allm)
        for t in range(nt):
            alls = alls + st[h, t, 1:2, :] * jnp.exp(st[h, t, 0:1, :] - allm)
        row = lax.broadcasted_iota(jnp.int32, (128, Rh), 0)
        back_t = jnp.where(row == 0, allm, alls).T
        factor = jnp.exp(tops[h] - back_t[:, 0:1]) / back_t[:, 1:2]

        @pl.loop(0, kn, unroll=True)
        def _(i):
            sl = pl.ds(pl.multiple_of(i * kstep, kstep), kstep)
            prob = lg[hs, sl] * factor
            cols = (lax.broadcasted_iota(jnp.int32, (Rh, kstep), 1) + i * kstep).astype(F32)
            target = (cols == local_label).astype(F32)
            sg[hs, sl] = (100.0 * (prob - target)).astype(BF16)

        @pl.loop(0, en, unroll=True)
        def _(i):
            sl = pl.ds(pl.multiple_of(i * estep, estep), estep)
            v = nn(sg[hs, :], tu[:, sl])
            bpart[hs, sl] = v
            bs[hs, sl] = v.astype(BF16)

        c_back[h] = exchange(BACK, lambda p: bs.at[rows_of(h, p), :], br.at[h, me], h)

    for h in both:
        own = rows_of(h, me)
        ugrad = bpart[own, :]
        finish(c_back[h])
        for o in range(1, nt):
            ugrad = ugrad + br[h, (me + o) % nt].astype(F32)
        along = jnp.sum(unit[h] * ugrad, axis=1, keepdims=True)
        emb_grad = ((ugrad - unit[h] * along) / emb_norm[h]).astype(BF16)
        out_grad[h] = norm_back(nt_dot(emb_grad, pj[...]) * gains[0:1, :], yhat[h], rstd_out[h])
        os_[h] = out_grad[h].astype(BF16)
        c_out[h] = exchange(OUTLOW, lambda p: os_.at[h], og.at[own, :], h)
        og[own, :] = os_[h]

    for h in both:
        hs = whole_half(h)
        finish(c_out[h])

        @pl.loop(0, hn, unroll=True)
        def _(i):
            sl = pl.ds(pl.multiple_of(i * hstep, hstep), hstep)
            ag[hs, sl] = (nt_dot(og[hs, :], wdf[sl, :]) * dgate[hs, sl]).astype(BF16)

        @pl.loop(0, dn, unroll=True)
        def _(i):
            sl = pl.ds(pl.multiple_of(i * dstep, dstep), dstep)
            v = nt_dot(ag[hs, :], wu[sl, :])
            part[hs, sl] = v
            ns[hs, sl] = v.astype(BF16)

        c_norm[h] = exchange(NORMED, lambda p: ns.at[rows_of(h, p), :], nr.at[h, me], h)

    for h in both:
        ngrad = part[rows_of(h, me), :]
        finish(c_norm[h])
        for o in range(1, nt):
            ngrad = ngrad + nr[h, (me + o) % nt].astype(F32)
        in_grad = out_grad[h] + norm_back(ngrad * pre_gain[...], xhat_own[h], rstd_in[h])
        rms = jnp.sqrt(jnp.mean(in_grad * in_grad, axis=1, keepdims=True) + 1e-06)
        delta = step_size[0] * in_grad / rms
        for t in range(nt):
            ds_[h, t] = delta[:, t * F:(t + 1) * F]
        land = pl.ds(pl.multiple_of(me * r + h * rh, rh), rh)
        c_fin[h] = exchange(FINAL, lambda p: ds_.at[h, p], dr.at[land, :], h)
        dr[land, :] = ds_[h, me]
    for h in both:
        finish(c_fin[h])
    out[...] = resid[...].astype(F32) + dr[...]


def solution(mesh):
    nd, nt = mesh.shape["dp"], mesh.shape["txt"]
    placed = (
        P("dp", "txt"),
        P(),
        P(),
        P("dp", "txt"),
        P("txt"),
        P("txt", "dp"),
        P(),
        P("txt"),
        P("txt"),
        P("txt", None),
        P("txt", None),
        P("dp"),
        P(),
    )

    def local(resid, pre_gain, pre_bias, up, up_bias, down, down_bias, post_gain, post_bias,
              projection, texts, labels, step_size):
        R, F = resid.shape
        D = nt * F
        Kd, H = up.shape
        E = projection.shape[1]
        T = texts.shape[0]
        r = R // nt
        NH = halves(r)
        rh, Rh = r // NH, R // NH
        V = pltpu.VMEM
        scratch = [
            V((nt, R, F), BF16),
            V((R, D), F32),
            V((R, D), BF16),
            V((D, H), BF16),
            V((nd, H, Kd), BF16),
            V((H, D), BF16),
            V((8, F), F32),
            V((nt, 8, F), F32),
            V((8, D), F32),
            V((D, E), BF16),
            V((T, E), BF16),
            V((R, H), BF16),
            V((R, H), F32),
            V((R, D), F32),
            V((R, D), BF16),
            V((NH, nt, rh, D), BF16),
            V((NH, rh, E), BF16),
            V((R, E), BF16),
            V((R, T), F32),
            V((R, T), BF16),
            V((NH, 8, Rh), F32),
            V((NH, nt, 8, Rh), F32),
            V((R, E), F32),
            V((R, E), BF16),
            V((NH, nt, rh, E), BF16),
            V((NH, rh, D), BF16),
            V((R, D), BF16),
            V((R, H), BF16),
            V((R, D), BF16),
            V((NH, nt, rh, D), BF16),
            V((NH, nt, rh, F), F32),
            V((R, F), F32),
            V((R, 128), F32),
            V((T, E), BF16),
            pltpu.SemaphoreType.DMA,
            pltpu.SemaphoreType.DMA((NH, 10, nt - 1)),
            pltpu.SemaphoreType.DMA((NH, 10, nt - 1)),
            pltpu.SemaphoreType.DMA((2, 2, nd // 2)),
            pltpu.SemaphoreType.DMA((2, 2, nd // 2)),
        ]
        vm = pl.BlockSpec(memory_space=pltpu.VMEM)
        line = lambda v: v.reshape(1, -1)
        return pl.pallas_call(
            functools.partial(kernel, nd, nt),
            out_shape=jax.ShapeDtypeStruct((R, F), F32),
            in_specs=[vm] * 10 + [pl.BlockSpec(memory_space=pl.ANY), vm] + [pl.BlockSpec(memory_space=pltpu.SMEM)],
            out_specs=vm,
            scratch_shapes=scratch,
            compiler_params=pltpu.CompilerParams(
                collective_id=0, has_side_effects=True, vmem_limit_bytes=60 * 1024 * 1024),
        )(resid, line(pre_gain), line(pre_bias), up, line(up_bias), down, line(down_bias),
          line(post_gain), line(post_bias), projection, texts, line(labels), step_size)

    return jax.shard_map(local, mesh=mesh, in_specs=placed, out_specs=P("dp", "txt"), check_vma=False)
```
